256 devices in a mesh: ka: 16 (over x, z_lo, core), grid: 16 (over y, z_hi).
Axes of the slice: x: 4, y: 4, z: 8 (z_hi: 4, z_lo: 2; z = z_hi * 2 + z_lo), core: 2. Of those that a mesh axis runs over, the one named last changes fastest.
Arguments:
- orbitals: bfloat16 [16, 2, 512, 16384], P('ka', None, None, 'grid'), may hold values from -6 to 6
- potential: float32 [3, 2, 16384], P(None, None, 'grid'), may hold values from -6 to 6
- partners: int32 [3, 16], replicated, may hold values from 0 to 15, each once within a row
- occupied: int32 [16], replicated, may hold values from 128 to 512
Outputs:
- sources: bfloat16 [3, 16, 2, 512, 16384], P(None, 'ka', None, None, 'grid')
- density: float32 [3, 16384], P(None, 'grid')
The draws below stay inside these ranges and needn't reach their ends.
Inputs may be any that keep to these rules, and one draw needn't show every extreme that they name: `partners`: each row is a permutation of the 16 k-points.
All inputs are finite; a program needn't handle non-finite values.
Results may differ from the reference program's by a relative error of at most 0.0051.
Values may be sent and summed in bfloat16 or wider, within the bound.
A program may use at most 128 MiB of HBM per device.

```python
import jax
import jax.numpy as jnp
from jax import lax

BANDS = 512
Q = 3
K = 16
GRID = 16384


def with_ends(result, own_key, smallest, high):
    place = [jax.random.randint(jax.random.fold_in(own_key, axis), (), 0, length) for axis, length in enumerate(result.shape)]
    longest = result.shape.index(max(result.shape))
    beside = place[:longest] + [(place[longest] + 1) % result.shape[longest]] + place[longest + 1:]
    return result.at[tuple(place)].set(smallest).at[tuple(beside)].set(high)


def level_of(stream_key, extent, split, smallest, high):
    loudness = 1.0
    for dim, shards_of in split:
        draws = jax.random.uniform(jax.random.fold_in(jax.random.fold_in(stream_key, 6), dim), (shards_of,), jnp.float32, smallest / len(split), high / len(split))
        loudness = loudness * jnp.repeat(jnp.exp(draws), extent[dim] // shards_of).reshape((-1,) + (1,) * (len(extent) - 1 - dim))
    return loudness


def noise(key, dims, scale, limit, split=(), kind=jnp.bfloat16):
    entries = scale * jax.random.normal(key, dims, jnp.float32)
    if split:
        entries = entries * level_of(key, dims, split, -0.22, 0.18)
    return jnp.clip(entries, -limit, limit).astype(kind)


def setup_inputs(seed: int = 0) -> dict:
    seeds = jax.random.split(jax.random.key(seed), 5)
    return {
        "orbitals": noise(seeds[0], (K, 2, BANDS, GRID), 1.0, 6.0, ((0, 16), (3, 16))),
        "potential": noise(seeds[1], (Q, 2, GRID), 1.0, 6.0, ((2, 16),), jnp.float32),
        "partners": jax.vmap(lambda own: jax.random.permutation(own, K))(jax.random.split(seeds[2], Q)).reshape((Q, K)).astype(jnp.int32),
        "occupied": with_ends(jax.random.randint(seeds[3], (K,), BANDS // 4, BANDS + 1), jax.random.fold_in(seeds[3], 1), BANDS // 4, BANDS).astype(jnp.int32),
    }


def reference(orbitals, potential, partners, occupied):
    volume_weight = 1.0 / GRID
    density_weight = 2.0 / (K * BANDS)
    band_ids = jnp.arange(BANDS, dtype=jnp.int32)
    all_sources = []
    all_density = []
    for q_index in range(Q):
        real_field = potential[q_index, 0]
        imag_field = potential[q_index, 1]

        def per_point(k_index):
            partner = partners[q_index, k_index]
            own_orbit = orbitals[k_index].astype(jnp.float32)
            partner_orbit = orbitals[partner].astype(jnp.float32)
            applied_real = real_field * own_orbit[0] - imag_field * own_orbit[1]
            applied_imag = real_field * own_orbit[1] + imag_field * own_orbit[0]
            rounded = lax.optimization_barrier(jnp.stack([applied_real, applied_imag]).astype(jnp.bfloat16))
            applied = rounded.astype(jnp.float32)
            swapped = jnp.stack([applied[1], -applied[0]])
            over_real = volume_weight * jnp.einsum("cmg,cng->mn", partner_orbit, applied)
            over_imag = volume_weight * jnp.einsum("cmg,cng->mn", partner_orbit, swapped)
            partner_mask = (band_ids < occupied[partner]).astype(jnp.float32)[:, None]
            masked = lax.optimization_barrier(jnp.stack([over_real * partner_mask, over_imag * partner_mask]).astype(jnp.bfloat16))
            masked = masked.astype(jnp.float32)
            weight_real = jnp.stack([masked[0], -masked[1]])
            weight_imag = jnp.stack([masked[1], masked[0]])
            projected_real = applied[0] - jnp.einsum("cmg,cmn->ng", partner_orbit, weight_real)
            projected_imag = applied[1] - jnp.einsum("cmg,cmn->ng", partner_orbit, weight_imag)
            source_block = jnp.stack([projected_real, projected_imag]).astype(jnp.bfloat16)
            own_mask = (band_ids < occupied[k_index]).astype(jnp.float32)[:, None]
            density_term = jnp.sum(own_mask * (own_orbit[0] * projected_real + own_orbit[1] * projected_imag), axis=0)
            return source_block, density_term

        source_blocks, density_terms = lax.map(per_point, jnp.arange(K, dtype=jnp.int32))
        all_sources.append(source_blocks)
        all_density.append(density_weight * jnp.sum(density_terms, axis=0))
    return jnp.stack(all_sources), jnp.stack(all_density)
```

```python
import functools

import jax
import jax.numpy as jnp
from jax import lax
from jax.experimental import pallas as pl
from jax.experimental.pallas import tpu as pltpu
from jax.sharding import PartitionSpec as P

MESH = pl.DeviceIdType.MESH
BLOCKS = 2


def remote(src, dst, send_sem, recv_sem, target):
    return pltpu.make_async_remote_copy(
        src_ref=src,
        dst_ref=dst,
        send_sem=send_sem,
        recv_sem=recv_sem,
        device_id=target,
        device_id_type=MESH,
    )


def dot(a, b, dims):
    return lax.dot_general(a, b, (dims, ((), ())), preferred_element_type=jnp.float32)


def kernel(
    sizes,
    partners,
    occupied,
    orbitals,
    potential,
    sources,
    density,
    held,
    picked,
    partner,
    applied,
    whole,
    ysend,
    yrecv,
    quarter,
    zsend,
    zrecv,
    masked,
    mixer,
    result,
    shares,
    sems,
):
    K, NY, NZ, Q, H = sizes
    _, _, B, G = orbitals.shape
    NX, J = K // 4, K // 2
    M = B // H
    R = M // J
    YN = B // NY
    ZN = YN // NZ
    volume_weight = 1.0 / (G * NY * NZ)
    density_weight = 2.0 / (K * B)
    units = [(q, h) for h in range(H) for q in range(Q)]

    ka = lax.axis_index("ka")
    gr = lax.axis_index("grid")
    x, low, core = lax.div(ka, 4), lax.rem(lax.div(ka, 2), 2), lax.rem(ka, 2)
    y, z = lax.div(gr, NZ), lax.rem(gr, NZ)

    order = [(0, 1)]
    for dx in [1, NX - 1, 2]:
        for dc in (0, 1):
            if 0 < dx < NX and (dx, dc) not in order:
                order.append((dx, dc))

    def plane(dx, dc):
        px, pc = lax.rem(x + dx + NX, NX), lax.rem(core + dc + 2, 2)
        return px * 4 + low * 2 + pc, px * 2 + pc

    mine = x * 2 + core
    beside = (x * 4 + (1 - low) * 2 + core, gr)

    def y_peer(d):
        return lax.rem(y + d, NY)

    def z_peer(d):
        return lax.rem(z + d, NZ)

    barrier = pltpu.get_barrier_semaphore()
    greeted = [(lax.rem(ka + d, K), gr) for d in range(1, K)]
    greeted += [(ka, y_peer(d) * NZ + z) for d in range(1, NY)]
    greeted += [(ka, y * NZ + z_peer(d)) for d in range(1, NZ)]
    for target in greeted:
        pl.semaphore_signal(barrier, inc=1, device_id=target, device_id_type=MESH)
    pl.semaphore_wait(barrier, len(greeted))

    def rows(h, piece):
        return pl.ds(pl.multiple_of(h * M + piece * R, R), R)

    for h in range(H):
        for i, (dx, dc) in enumerate(order):
            pk, pj = plane(dx, dc)
            remote(
                orbitals.at[0, :, rows(h, pj), :],
                held[h].at[ka],
                sems["spread_s"].at[h],
                sems["spread_r"].at[h, i],
                (pk, gr),
            ).start()

    def apply_field(q):
        real, imag = potential[q, 0:1, :], potential[q, 1:2, :]

        def strip(t, _):
            at = pl.ds(pl.multiple_of(t * 64, 64), 64)
            under = pl.ds(pl.multiple_of(B + t * 64, 64), 64)
            own_real = orbitals[0, 0, at, :].astype(jnp.float32)
            own_imag = orbitals[0, 1, at, :].astype(jnp.float32)
            applied[q, at, :] = (real * own_real - imag * own_imag).astype(jnp.bfloat16)
            applied[q, under, :] = (real * own_imag + imag * own_real).astype(jnp.bfloat16)
            return 0

        lax.fori_loop(0, B // 64, strip, 0)

    def relay(h, slot, source):
        remote(
            source, held[h].at[slot], sems["relay_s"].at[h], sems["relay_r"].at[h], beside
        ).start()

    for h in range(H):
        relay(h, ka, orbitals.at[0, :, rows(h, mine), :])
        held[h][ka] = orbitals[0, :, rows(h, mine), :]
        for q in range(Q):
            if q % H == h:
                apply_field(q)
        for i, (dx, dc) in enumerate(order):
            slot, _ = plane(-dx, -dc)
            remote(
                held[h].at[slot],
                held[h].at[slot],
                sems["spread_s"].at[h],
                sems["spread_r"].at[h, i],
                beside,
            ).wait_recv()
            relay(h, slot, held[h].at[slot])

    def wait_relay(h):
        block = held[h].at[pl.ds(0, J)]
        remote(block, block, sems["relay_s"].at[h], sems["relay_r"].at[h], beside).wait_recv()

    def hand_out(h):
        for q in range(Q):
            u = h * Q + q
            for i, (dx, dc) in enumerate(order):
                pk, _ = plane(dx, dc)
                picked[u, i] = held[h][partners[q, pk]]
            partner[q, :, rows(h, mine), :] = held[h][partners[q, ka]]
            for i, (dx, dc) in enumerate(order):
                pk, _ = plane(dx, dc)
                remote(
                    picked.at[u, i],
                    partner.at[q, :, rows(h, mine), :],
                    sems["hand_s"].at[u],
                    sems["hand_r"].at[u],
                    (pk, gr),
                ).start()

    def intersect(u):
        q, h = units[u]
        block = partner.at[q, :, pl.ds(h * M, (J - 1) * R), :]
        remote(block, block, sems["hand_s"].at[u], sems["hand_r"].at[u], beside).wait_recv()
        last = ((1,), (1,))
        field = applied[q]
        with_real = dot(field, partner[q, 0, h * M : (h + 1) * M, :], last)
        with_imag = dot(field, partner[q, 1, h * M : (h + 1) * M, :], last)
        real = volume_weight * (with_real[:B] + with_imag[B:])
        imag = volume_weight * (with_real[B:] - with_imag[:B])
        for part, value in enumerate((real, imag)):
            value = value.reshape(NY, YN, M)
            whole[:, part] = value
            ysend[u, :, part] = value.astype(jnp.bfloat16)
        for d in range(1, NY):
            remote(
                ysend.at[u, y_peer(d)],
                yrecv.at[u, d - 1],
                sems["y_s"].at[u],
                sems["y_r"].at[u],
                (ka, y_peer(d) * NZ + z),
            ).start()

    def sum_y(u):
        if NY > 1:
            block = yrecv.at[u]
            remote(block, block, sems["y_s"].at[u], sems["y_r"].at[u], beside).wait_recv()
        for t in range(NZ):
            value = whole[y, :, t * ZN : (t + 1) * ZN, :]
            for d in range(NY - 1):
                value = value + yrecv[u, d, :, t * ZN : (t + 1) * ZN, :].astype(jnp.float32)
            quarter[t] = value
            zsend[u, t] = value.astype(jnp.bfloat16)
        for d in range(1, NZ):
            remote(
                zsend.at[u, z_peer(d)],
                zrecv.at[u, d - 1],
                sems["z_s"].at[u],
                sems["z_r"].at[u],
                (ka, y * NZ + z_peer(d)),
            ).start()

    def sum_z(u):
        q, h = units[u]
        if NZ > 1:
            block = zrecv.at[u]
            remote(block, block, sems["z_s"].at[u], sems["z_r"].at[u], beside).wait_recv()
        value = quarter[z]
        for d in range(NZ - 1):
            value = value + zrecv[u, d].astype(jnp.float32)
        bands = h * M + lax.broadcasted_iota(jnp.int32, value.shape, 2)
        count = occupied[partners[q, ka]]
        masked[u, y, z] = jnp.where(bands < count, value, 0.0).astype(jnp.bfloat16)
        for d in range(1, NZ):
            remote(
                masked.at[u, y, z],
                masked.at[u, y, z],
                sems["zz_s"].at[u],
                sems["zz_r"].at[u],
                (ka, y * NZ + z_peer(d)),
            ).start()

    def gather_z(u):
        if NZ > 1:
            block = masked.at[u, 0, pl.ds(0, NZ - 1)]
            remote(block, block, sems["zz_s"].at[u], sems["zz_r"].at[u], beside).wait_recv()
        for d in range(1, NY):
            remote(
                masked.at[u, y],
                masked.at[u, y],
                sems["yy_s"].at[u],
                sems["yy_r"].at[u],
                (ka, y_peer(d) * NZ + z),
            ).start()

    def gather_y(u):
        q, h = units[u]
        if NY > 1:
            block = masked.at[u, pl.ds(0, NY - 1)]
            remote(block, block, sems["yy_s"].at[u], sems["yy_r"].at[u], beside).wait_recv()
        real = masked[u, :, :, 0].reshape(B, M)
        imag = masked[u, :, :, 1].reshape(B, M)
        mixer[q, 0:B, h * M : (h + 1) * M] = real
        mixer[q, 0:B, B + h * M : B + (h + 1) * M] = -imag
        mixer[q, B : 2 * B, h * M : (h + 1) * M] = imag
        mixer[q, B : 2 * B, B + h * M : B + (h + 1) * M] = real

    def out_copy(q):
        return pltpu.make_async_copy(result.at[q], sources.at[q, 0], sems["out"].at[q])

    def project(q):
        own_count = occupied[ka]
        width = 256

        def strip(t, _):
            at = pl.ds(pl.multiple_of(t * width, width), width)
            mixed = dot(mixer[q], partner[q, :, :, at].reshape(2 * B, width), ((1,), (0,)))
            real = applied[q, 0:B, at].astype(jnp.float32) - mixed[:B]
            imag = applied[q, B : 2 * B, at].astype(jnp.float32) - mixed[B:]
            result[q, 0, :, at] = real.astype(jnp.bfloat16)
            result[q, 1, :, at] = imag.astype(jnp.bfloat16)
            term = orbitals[0, 0, :, at].astype(jnp.float32) * real
            term = term + orbitals[0, 1, :, at].astype(jnp.float32) * imag
            bands = lax.broadcasted_iota(jnp.int32, term.shape, 0)
            term = jnp.where(bands < own_count, term, 0.0)
            shares[q, ka, :, at] = density_weight * jnp.sum(term, axis=0, keepdims=True)
            return 0

        lax.fori_loop(0, G // width, strip, 0)
        out_copy(q).start()
        for d in range(1, K):
            remote(
                shares.at[q, ka],
                shares.at[q, ka],
                sems["share_s"].at[q],
                sems["share_r"].at[q],
                (lax.rem(ka + d, K), gr),
            ).start()

    wait_relay(0)
    hand_out(0)
    count = len(units)
    for u in range(count + 2):
        if u < count:
            intersect(u)
        if 1 <= u <= count:
            sum_z(u - 1)
        if 2 <= u:
            gather_y(u - 2)
            q, h = units[u - 2]
            if h == H - 1:
                project(q)
        if 1 <= u <= count:
            gather_z(u - 1)
        if u < count:
            sum_y(u)
        if u % Q == 1 and u // Q + 1 < H:
            wait_relay(u // Q + 1)
            hand_out(u // Q + 1)

    for q in range(Q):
        block = shares.at[q, pl.ds(0, K - 1)]
        remote(block, block, sems["share_s"].at[q], sems["share_r"].at[q], beside).wait_recv()
        density[q : q + 1, :] = jnp.sum(shares[q], axis=0)

    def sent(block, sem):
        remote(block, block, sem, sem, beside).wait_send()

    for q in range(Q):
        out_copy(q).wait()
        sent(shares.at[q, pl.ds(0, K - 1)], sems["share_s"].at[q])
    for h in range(H):
        sent(held[h].at[pl.ds(0, J - 1)], sems["spread_s"].at[h])
        sent(held[h].at[pl.ds(0, J)], sems["relay_s"].at[h])
    for u in range(count):
        sent(picked.at[u], sems["hand_s"].at[u])
        if NY > 1:
            sent(yrecv.at[u], sems["y_s"].at[u])
            sent(masked.at[u, pl.ds(0, NY - 1)], sems["yy_s"].at[u])
        if NZ > 1:
            sent(zrecv.at[u], sems["z_s"].at[u])
            sent(masked.at[u, 0, pl.ds(0, NZ - 1)], sems["zz_s"].at[u])


def shards(sizes, orbitals, potential, partners, occupied):
    K, NY, NZ, Q, H = sizes
    _, _, B, G = orbitals.shape
    J, M = K // 2, B // H
    R, YN = M // J, B // NY
    ZN, U = YN // NZ, Q * H
    half, full = jnp.bfloat16, jnp.float32
    DMA = pltpu.SemaphoreType.DMA
    sems = {name: DMA((U,)) for part in ("hand", "y", "z", "zz", "yy") for name in (part + "_s", part + "_r")}
    sems |= {"spread_s": DMA((H,)), "spread_r": DMA((H, J)), "relay_s": DMA((H,)), "relay_r": DMA((H,))}
    sems |= {"share_s": DMA((Q,)), "share_r": DMA((Q,)), "out": DMA((Q,))}
    scratch = dict(
        held=[pltpu.VMEM((K, 2, R, G), half) for _ in range(H)],
        picked=pltpu.VMEM((U, J - 1, 2, R, G), half),
        partner=pltpu.VMEM((Q, 2, B, G), half),
        applied=pltpu.VMEM((Q, 2 * B, G), half),
        whole=pltpu.VMEM((NY, 2, YN, M), full),
        ysend=pltpu.VMEM((U, NY, 2, YN, M), half),
        yrecv=pltpu.VMEM((U, max(NY - 1, 1), 2, YN, M), half),
        quarter=pltpu.VMEM((NZ, 2, ZN, M), full),
        zsend=pltpu.VMEM((U, NZ, 2, ZN, M), half),
        zrecv=pltpu.VMEM((U, max(NZ - 1, 1), 2, ZN, M), half),
        masked=pltpu.VMEM((U, NY, NZ, 2, ZN, M), half),
        mixer=pltpu.VMEM((Q, 2 * B, 2 * B), half),
        result=pltpu.VMEM((Q, 2, B, G), half),
        shares=pltpu.VMEM((Q, K, 1, G), full),
        sems=sems,
    )
    vmem = pl.BlockSpec(memory_space=pltpu.VMEM)
    smem = pl.BlockSpec(memory_space=pltpu.SMEM)
    return pl.pallas_call(
        functools.partial(kernel, sizes),
        out_shape=(
            jax.ShapeDtypeStruct((Q, 1, 2, B, G), half),
            jax.ShapeDtypeStruct((Q, G), full),
        ),
        in_specs=[smem, smem, vmem, vmem],
        out_specs=(pl.BlockSpec(memory_space=pl.ANY), vmem),
        scratch_shapes=scratch,
        compiler_params=pltpu.CompilerParams(
            collective_id=0, has_side_effects=True, vmem_limit_bytes=64 * 1024 * 1024 - 65536
        ),
    )(partners, occupied, orbitals, potential)


def solution(mesh, ways=None):
    K, points = mesh.shape["ka"], mesh.shape["grid"]
    NY, NZ = ways or (4, points // 4)

    def local(orbitals, potential, partners, occupied):
        sizes = (K, NY, NZ, potential.shape[0], BLOCKS)
        return shards(sizes, orbitals, potential, partners, occupied)

    return jax.shard_map(
        local,
        mesh=mesh,
        in_specs=(P("ka", None, None, "grid"), P(None, None, "grid"), P(), P()),
        out_specs=(P(None, "ka", None, None, "grid"), P(None, "grid")),
        check_vma=False,
    )
```

```python
import functools

import jax
import jax.numpy as jnp
from jax import lax
from jax.experimental import pallas as pl
from jax.experimental.pallas import tpu as pltpu
from jax.sharding import PartitionSpec as P

MESH = pl.DeviceIdType.MESH
BLOCKS = 4
LAGS = (7.0, 13.0, 19.5, 26.0)


def remote(src, dst, send_sem, recv_sem, target):
    return pltpu.make_async_remote_copy(
        src_ref=src,
        dst_ref=dst,
        send_sem=send_sem,
        recv_sem=recv_sem,
        device_id=target,
        device_id_type=MESH,
    )


def dot(a, b, dims):
    return lax.dot_general(a, b, (dims, ((), ())), preferred_element_type=jnp.float32)


def kernel(
    sizes,
    partners,
    occupied,
    orbitals,
    potential,
    sources,
    density,
    held,
    picked,
    partner,
    applied,
    whole,
    ysend,
    yrecv,
    quarter,
    zsend,
    zrecv,
    masked,
    mixer,
    shares,
    sems,
):
    K, NY, NZ, Q, H = sizes
    _, _, B, G = orbitals.shape
    NX, J = K // 4, K // 2
    M = B // H
    R = M // J
    YN = B // NY
    ZN = YN // NZ
    volume_weight = 1.0 / (G * NY * NZ)
    density_weight = 2.0 / (K * B)
    units = [(q, h) for h in range(H) for q in range(Q)]

    ka = lax.axis_index("ka")
    gr = lax.axis_index("grid")
    x, low, core = lax.div(ka, 4), lax.rem(lax.div(ka, 2), 2), lax.rem(ka, 2)
    y, z = lax.div(gr, NZ), lax.rem(gr, NZ)

    order = [(0, 1)]
    for dx in [1, NX - 1, 2]:
        for dc in (0, 1):
            if 0 < dx < NX and (dx, dc) not in order:
                order.append((dx, dc))

    def plane(dx, dc):
        px, pc = lax.rem(x + dx + NX, NX), lax.rem(core + dc + 2, 2)
        return px * 4 + low * 2 + pc, px * 2 + pc

    mine = x * 2 + core
    beside = (x * 4 + (1 - low) * 2 + core, gr)

    def y_peer(d):
        return lax.rem(y + d, NY)

    def z_peer(d):
        return lax.rem(z + d, NZ)

    barrier = pltpu.get_barrier_semaphore()
    greeted = [(lax.rem(ka + d, K), gr) for d in range(1, K)]
    greeted += [(ka, y_peer(d) * NZ + z) for d in range(1, NY)]
    greeted += [(ka, y * NZ + z_peer(d)) for d in range(1, NZ)]
    for target in greeted:
        pl.semaphore_signal(barrier, inc=1, device_id=target, device_id_type=MESH)
    pl.semaphore_wait(barrier, len(greeted))

    def rows(h, piece):
        return pl.ds(pl.multiple_of(h * M + piece * R, R), R)

    for h in range(H):
        for i, (dx, dc) in enumerate(order):
            pk, pj = plane(dx, dc)
            remote(
                orbitals.at[0, :, rows(h, pj), :],
                held[h].at[ka],
                sems["spread_s"].at[h],
                sems["spread_r"].at[h, i],
                (pk, gr),
            ).start()

    def apply_field(q):
        real, imag = potential[q, 0:1, :], potential[q, 1:2, :]

        def strip(t, _):
            at = pl.ds(pl.multiple_of(t * 64, 64), 64)
            under = pl.ds(pl.multiple_of(B + t * 64, 64), 64)
            own_real = orbitals[0, 0, at, :].astype(jnp.float32)
            own_imag = orbitals[0, 1, at, :].astype(jnp.float32)
            applied[q, at, :] = (real * own_real - imag * own_imag).astype(jnp.bfloat16)
            applied[q, under, :] = (real * own_imag + imag * own_real).astype(jnp.bfloat16)
            return 0

        lax.fori_loop(0, B // 64, strip, 0)

    def relay(h, slot, source):
        remote(
            source, held[h].at[slot], sems["relay_s"].at[h], sems["relay_r"].at[h], beside
        ).start()

    def start_relay(h):
        relay(h, ka, orbitals.at[0, :, rows(h, mine), :])
        held[h][ka] = orbitals[0, :, rows(h, mine), :]

    def pass_on(h):
        for i, (dx, dc) in enumerate(order):
            slot, _ = plane(-dx, -dc)
            remote(
                held[h].at[slot],
                held[h].at[slot],
                sems["spread_s"].at[h],
                sems["spread_r"].at[h, i],
                beside,
            ).wait_recv()
            relay(h, slot, held[h].at[slot])

    def wait_relay(h):
        block = held[h].at[pl.ds(0, J)]
        remote(block, block, sems["relay_s"].at[h], sems["relay_r"].at[h], beside).wait_recv()

    def hand_out(h):
        for q in range(Q):
            u = h * Q + q
            for i, (dx, dc) in enumerate(order):
                pk, _ = plane(dx, dc)
                picked[u, i] = held[h][partners[q, pk]]
            partner[q, :, rows(h, mine), :] = held[h][partners[q, ka]]
            for i, (dx, dc) in enumerate(order):
                pk, _ = plane(dx, dc)
                remote(
                    picked.at[u, i],
                    partner.at[q, :, rows(h, mine), :],
                    sems["hand_s"].at[u],
                    sems["hand_r"].at[u],
                    (pk, gr),
                ).start()

    def intersect(u):
        q, h = units[u]
        block = partner.at[q, :, pl.ds(h * M, (J - 1) * R), :]
        remote(block, block, sems["hand_s"].at[u], sems["hand_r"].at[u], beside).wait_recv()
        last = ((1,), (1,))
        orbits = partner[q, :, h * M : (h + 1) * M, :].reshape(2 * M, G)
        both = dot(applied[q], orbits, last)
        real = volume_weight * (both[:B, :M] + both[B:, M:])
        imag = volume_weight * (both[B:, :M] - both[:B, M:])
        for part, value in enumerate((real, imag)):
            value = value.reshape(NY, YN, M)
            whole[u % 3, :, part] = value
            ysend[u, :, part] = value.astype(jnp.bfloat16)
        for d in range(1, NY):
            remote(
                ysend.at[u, y_peer(d)],
                yrecv.at[u, d - 1],
                sems["y_s"].at[u],
                sems["y_r"].at[u],
                (ka, y_peer(d) * NZ + z),
            ).start()

    def sum_y(u):
        if NY > 1:
            block = yrecv.at[u]
            remote(block, block, sems["y_s"].at[u], sems["y_r"].at[u], beside).wait_recv()
        for t in range(NZ):
            value = whole[u % 3, y, :, t * ZN : (t + 1) * ZN, :]
            for d in range(NY - 1):
                value = value + yrecv[u, d, :, t * ZN : (t + 1) * ZN, :].astype(jnp.float32)
            quarter[u % 3, t] = value
            zsend[u, t] = value.astype(jnp.bfloat16)
        for d in range(1, NZ):
            remote(
                zsend.at[u, z_peer(d)],
                zrecv.at[u, d - 1],
                sems["z_s"].at[u],
                sems["z_r"].at[u],
                (ka, y * NZ + z_peer(d)),
            ).start()

    def sum_z(u):
        q, h = units[u]
        if NZ > 1:
            block = zrecv.at[u]
            remote(block, block, sems["z_s"].at[u], sems["z_r"].at[u], beside).wait_recv()
        value = quarter[u % 3, z]
        for d in range(NZ - 1):
            value = value + zrecv[u, d].astype(jnp.float32)
        bands = h * M + lax.broadcasted_iota(jnp.int32, value.shape, 2)
        count = occupied[partners[q, ka]]
        masked[u, y, z] = jnp.where(bands < count, value, 0.0).astype(jnp.bfloat16)
        for d in range(1, NZ):
            remote(
                masked.at[u, y, z],
                masked.at[u, y, z],
                sems["zz_s"].at[u],
                sems["zz_r"].at[u],
                (ka, y * NZ + z_peer(d)),
            ).start()

    def gather_z(u):
        if NZ > 1:
            block = masked.at[u, 0, pl.ds(0, NZ - 1)]
            remote(block, block, sems["zz_s"].at[u], sems["zz_r"].at[u], beside).wait_recv()
        for d in range(1, NY):
            remote(
                masked.at[u, y],
                masked.at[u, y],
                sems["yy_s"].at[u],
                sems["yy_r"].at[u],
                (ka, y_peer(d) * NZ + z),
            ).start()

    def gather_y(u):
        q, h = units[u]
        if NY > 1:
            block = masked.at[u, pl.ds(0, NY - 1)]
            remote(block, block, sems["yy_s"].at[u], sems["yy_r"].at[u], beside).wait_recv()
        real = masked[u, :, :, 0].reshape(B, M)
        imag = masked[u, :, :, 1].reshape(B, M)
        mixer[q, 0:B, h * M : (h + 1) * M] = real
        mixer[q, 0:B, B + h * M : B + (h + 1) * M] = -imag
        mixer[q, B : 2 * B, h * M : (h + 1) * M] = imag
        mixer[q, B : 2 * B, B + h * M : B + (h + 1) * M] = real

    def project(q):
        own_count = occupied[ka]
        width = 256

        def strip(t, _):
            at = pl.ds(pl.multiple_of(t * width, width), width)
            mixed = dot(mixer[q], partner[q, :, :, at].reshape(2 * B, width), ((1,), (0,)))
            real = applied[q, 0:B, at].astype(jnp.float32) - mixed[:B]
            imag = applied[q, B : 2 * B, at].astype(jnp.float32) - mixed[B:]
            sources[q, 0, 0, :, at] = real.astype(jnp.bfloat16)
            sources[q, 0, 1, :, at] = imag.astype(jnp.bfloat16)
            term = orbitals[0, 0, :, at].astype(jnp.float32) * real
            term = term + orbitals[0, 1, :, at].astype(jnp.float32) * imag
            bands = lax.broadcasted_iota(jnp.int32, term.shape, 0)
            term = jnp.where(bands < own_count, term, 0.0)
            shares[q, ka, :, at] = density_weight * jnp.sum(term, axis=0, keepdims=True)
            return 0

        lax.fori_loop(0, G // width, strip, 0)
        for d in range(1, K):
            remote(
                shares.at[q, ka],
                shares.at[q, ka],
                sems["share_s"].at[q],
                sems["share_r"].at[q],
                (lax.rem(ka + d, K), gr),
            ).start()

    def finish(u):
        gather_y(u)
        q, h = units[u]
        if h == H - 1:
            project(q)

    def give(h):
        wait_relay(h)
        hand_out(h)

    count = len(units)
    start_relay(0)
    apply_field(0)
    beat = 22.0 / H
    first = 30 + beat
    steps = [(13 + beat * h, 0, pass_on, h) for h in range(H)]
    steps += [(7 + 2 * beat * (h + 1), 1, give, h) for h in range(H)]
    steps += [(6 + beat * h, 2, start_relay, h) for h in range(1, H)]
    steps += [(7 + beat * q, 3, apply_field, q) for q in range(1, Q)]
    for u in range(count):
        arrives = first + beat * u
        steps += [(arrives, 4, intersect, u)]
        for i, (lag, step) in enumerate(zip(LAGS, (sum_y, sum_z, gather_z, finish))):
            steps += [(arrives + lag, 5 + i, step, u)]
    for _, _, step, argument in sorted(steps, key=lambda entry: entry[:2] + entry[3:]):
        step(argument)

    for q in range(Q):
        block = shares.at[q, pl.ds(0, K - 1)]
        remote(block, block, sems["share_s"].at[q], sems["share_r"].at[q], beside).wait_recv()
        density[q : q + 1, :] = jnp.sum(shares[q], axis=0)

    def sent(block, sem):
        remote(block, block, sem, sem, beside).wait_send()

    for q in range(Q):
        sent(shares.at[q, pl.ds(0, K - 1)], sems["share_s"].at[q])
    for h in range(H):
        sent(held[h].at[pl.ds(0, J - 1)], sems["spread_s"].at[h])
        sent(held[h].at[pl.ds(0, J)], sems["relay_s"].at[h])
    for u in range(count):
        sent(picked.at[u], sems["hand_s"].at[u])
        if NY > 1:
            sent(yrecv.at[u], sems["y_s"].at[u])
            sent(masked.at[u, pl.ds(0, NY - 1)], sems["yy_s"].at[u])
        if NZ > 1:
            sent(zrecv.at[u], sems["z_s"].at[u])
            sent(masked.at[u, 0, pl.ds(0, NZ - 1)], sems["zz_s"].at[u])


def shards(sizes, orbitals, potential, partners, occupied):
    K, NY, NZ, Q, H = sizes
    _, _, B, G = orbitals.shape
    J, M = K // 2, B // H
    R, YN = M // J, B // NY
    ZN, U = YN // NZ, Q * H
    half, full = jnp.bfloat16, jnp.float32
    DMA = pltpu.SemaphoreType.DMA
    sems = {name: DMA((U,)) for part in ("hand", "y", "z", "zz", "yy") for name in (part + "_s", part + "_r")}
    sems |= {"spread_s": DMA((H,)), "spread_r": DMA((H, J)), "relay_s": DMA((H,)), "relay_r": DMA((H,))}
    sems |= {"share_s": DMA((Q,)), "share_r": DMA((Q,))}
    scratch = dict(
        held=[pltpu.VMEM((K, 2, R, G), half) for _ in range(H)],
        picked=pltpu.VMEM((U, J - 1, 2, R, G), half),
        partner=pltpu.VMEM((Q, 2, B, G), half),
        applied=pltpu.VMEM((Q, 2 * B, G), half),
        whole=pltpu.VMEM((3, NY, 2, YN, M), full),
        ysend=pltpu.VMEM((U, NY, 2, YN, M), half),
        yrecv=pltpu.VMEM((U, max(NY - 1, 1), 2, YN, M), half),
        quarter=pltpu.VMEM((3, NZ, 2, ZN, M), full),
        zsend=pltpu.VMEM((U, NZ, 2, ZN, M), half),
        zrecv=pltpu.VMEM((U, max(NZ - 1, 1), 2, ZN, M), half),
        masked=pltpu.VMEM((U, NY, NZ, 2, ZN, M), half),
        mixer=pltpu.VMEM((Q, 2 * B, 2 * B), half),
        shares=pltpu.VMEM((Q, K, 1, G), full),
        sems=sems,
    )
    vmem = pl.BlockSpec(memory_space=pltpu.VMEM)
    smem = pl.BlockSpec(memory_space=pltpu.SMEM)
    return pl.pallas_call(
        functools.partial(kernel, sizes),
        out_shape=(
            pltpu.VMEM((Q, 1, 2, B, G), half),
            pltpu.VMEM((Q, G), full),
        ),
        in_specs=[smem, smem, vmem, vmem],
        out_specs=(vmem, vmem),
        scratch_shapes=scratch,
        compiler_params=pltpu.CompilerParams(
            collective_id=0, has_side_effects=True, vmem_limit_bytes=54 * 1024 * 1024
        ),
    )(partners, occupied, orbitals, potential)


def solution(mesh, ways=None):
    K, points = mesh.shape["ka"], mesh.shape["grid"]
    NY, NZ = ways or (4, points // 4)

    def local(orbitals, potential, partners, occupied):
        sizes = (K, NY, NZ, potential.shape[0], BLOCKS)
        return shards(sizes, orbitals, potential, partners, occupied)

    return jax.shard_map(
        local,
        mesh=mesh,
        in_specs=(P("ka", None, None, "grid"), P(None, None, "grid"), P(), P()),
        out_specs=(P(None, "ka", None, None, "grid"), P(None, "grid")),
        check_vma=False,
    )
```

```python
import functools

import jax
import jax.numpy as jnp
from jax import lax
from jax.experimental import pallas as pl
from jax.experimental.pallas import tpu as pltpu
from jax.sharding import PartitionSpec as P

MESH = pl.DeviceIdType.MESH
BLOCKS = 4
LAGS = (10.0, 17.0, 25.0)
GATHERED = 35.0
LAST = (26.0, 30.0, 34.0)


def remote(src, dst, send_sem, recv_sem, target):
    return pltpu.make_async_remote_copy(
        src_ref=src,
        dst_ref=dst,
        send_sem=send_sem,
        recv_sem=recv_sem,
        device_id=target,
        device_id_type=MESH,
    )


def dot(a, b, dims):
    return lax.dot_general(a, b, (dims, ((), ())), preferred_element_type=jnp.float32)


def kernel(
    sizes,
    given_partners,
    given_occupied,
    given_orbitals,
    given_potential,
    sources,
    density,
    partners,
    occupied,
    potential,
    orbitals,
    held,
    picked,
    partner,
    applied,
    whole,
    ysend,
    yrecv,
    quarter,
    zsend,
    zrecv,
    masked,
    mixer,
    part,
    shares,
    sems,
):
    K, NY, NZ, Q, H = sizes
    _, B, G = orbitals.shape
    NX, J = K // 4, K // 2
    M = B // H
    R = M // J
    YN = B // NY
    ZN = YN // NZ
    volume_weight = 1.0 / (G * NY * NZ)
    density_weight = 2.0 / (K * B)
    units = [(q, h) for h in range(H) for q in range(Q)]

    ka = lax.axis_index("ka")
    gr = lax.axis_index("grid")
    x, low, core = lax.div(ka, 4), lax.rem(lax.div(ka, 2), 2), lax.rem(ka, 2)
    y, z = lax.div(gr, NZ), lax.rem(gr, NZ)

    order = [(0, 1)]
    for dx in [1, NX - 1, 2]:
        for dc in (0, 1):
            if 0 < dx < NX and (dx, dc) not in order:
                order.append((dx, dc))

    def plane(dx, dc):
        px, pc = lax.rem(x + dx + NX, NX), lax.rem(core + dc + 2, 2)
        return px * 4 + low * 2 + pc, px * 2 + pc

    mine = x * 2 + core
    beside = (x * 4 + (1 - low) * 2 + core, gr)

    def y_peer(d):
        return lax.rem(y + d, NY)

    def z_peer(d):
        return lax.rem(z + d, NZ)

    barrier = pltpu.get_barrier_semaphore()
    greeted = [(lax.rem(ka + d, K), gr) for d in range(1, K)]
    greeted += [(ka, y_peer(d) * NZ + z) for d in range(1, NY)]
    greeted += [(ka, y * NZ + z_peer(d)) for d in range(1, NZ)]
    for target in greeted:
        pl.semaphore_signal(barrier, inc=1, device_id=target, device_id_type=MESH)
    loads = [
        pltpu.make_async_copy(src, dst, sems["load"].at[i])
        for i, (src, dst) in enumerate(
            [
                (given_orbitals.at[0], orbitals),
                (given_potential, potential),
                (given_partners, partners),
                (given_occupied, occupied),
            ]
        )
    ]
    for load in loads:
        load.start()
    pl.semaphore_wait(barrier, len(greeted))
    loads[0].wait()

    def rows(h, piece):
        return pl.ds(pl.multiple_of(h * M + piece * R, R), R)

    for h in range(H):
        for i, (dx, dc) in enumerate(order):
            pk, pj = plane(dx, dc)
            remote(
                orbitals.at[:, rows(h, pj), :],
                held[h].at[ka],
                sems["spread_s"].at[h],
                sems["spread_r"].at[h, i],
                (pk, gr),
            ).start()

    def apply_field(q):
        real, imag = potential[q, 0:1, :], potential[q, 1:2, :]

        def strip(t, _):
            at = pl.ds(pl.multiple_of(t * 64, 64), 64)
            under = pl.ds(pl.multiple_of(B + t * 64, 64), 64)
            own_real = orbitals[0, at, :].astype(jnp.float32)
            own_imag = orbitals[1, at, :].astype(jnp.float32)
            applied[q, at, :] = (real * own_real - imag * own_imag).astype(jnp.bfloat16)
            applied[q, under, :] = (real * own_imag + imag * own_real).astype(jnp.bfloat16)
            return 0

        lax.fori_loop(0, B // 64, strip, 0)

    def relay(h, slot, source):
        remote(
            source, held[h].at[slot], sems["relay_s"].at[h], sems["relay_r"].at[h], beside
        ).start()

    def start_relay(h):
        relay(h, ka, orbitals.at[:, rows(h, mine), :])
        held[h][ka] = orbitals[:, rows(h, mine), :]

    def pass_on(h):
        for i, (dx, dc) in enumerate(order):
            slot, _ = plane(-dx, -dc)
            remote(
                held[h].at[slot],
                held[h].at[slot],
                sems["spread_s"].at[h],
                sems["spread_r"].at[h, i],
                beside,
            ).wait_recv()
            relay(h, slot, held[h].at[slot])

    def wait_relay(h):
        block = held[h].at[pl.ds(0, J)]
        remote(block, block, sems["relay_s"].at[h], sems["relay_r"].at[h], beside).wait_recv()

    def hand_out(h):
        for q in range(Q):
            u = h * Q + q
            for i, (dx, dc) in enumerate(order):
                pk, _ = plane(dx, dc)
                picked[u, i] = held[h][partners[q, pk]]
            partner[q, :, rows(h, mine), :] = held[h][partners[q, ka]]
            for i, (dx, dc) in enumerate(order):
                pk, _ = plane(dx, dc)
                remote(
                    picked.at[u, i],
                    partner.at[q, :, rows(h, mine), :],
                    sems["hand_s"].at[u],
                    sems["hand_r"].at[u],
                    (pk, gr),
                ).start()

    def intersect(u):
        q, h = units[u]
        block = partner.at[q, :, pl.ds(h * M, (J - 1) * R), :]
        remote(block, block, sems["hand_s"].at[u], sems["hand_r"].at[u], beside).wait_recv()
        last = ((1,), (1,))
        orbits = partner[q, :, h * M : (h + 1) * M, :].reshape(2 * M, G)
        both = dot(applied[q], orbits, last)
        real = volume_weight * (both[:B, :M] + both[B:, M:])
        imag = volume_weight * (both[B:, :M] - both[:B, M:])
        for part, value in enumerate((real, imag)):
            value = value.reshape(NY, YN, M)
            whole[u % 3, :, part] = value
            ysend[u, :, part] = value.astype(jnp.bfloat16)
        for d in range(1, NY):
            remote(
                ysend.at[u, y_peer(d)],
                yrecv.at[u, d - 1],
                sems["y_s"].at[u],
                sems["y_r"].at[u],
                (ka, y_peer(d) * NZ + z),
            ).start()

    def sum_y(u):
        if NY > 1:
            block = yrecv.at[u]
            remote(block, block, sems["y_s"].at[u], sems["y_r"].at[u], beside).wait_recv()
        for t in range(NZ):
            value = whole[u % 3, y, :, t * ZN : (t + 1) * ZN, :]
            for d in range(NY - 1):
                value = value + yrecv[u, d, :, t * ZN : (t + 1) * ZN, :].astype(jnp.float32)
            quarter[u % 3, t] = value
            zsend[u, t] = value.astype(jnp.bfloat16)
        for d in range(1, NZ):
            remote(
                zsend.at[u, z_peer(d)],
                zrecv.at[u, d - 1],
                sems["z_s"].at[u],
                sems["z_r"].at[u],
                (ka, y * NZ + z_peer(d)),
            ).start()

    def sum_z(u):
        q, h = units[u]
        if NZ > 1:
            block = zrecv.at[u]
            remote(block, block, sems["z_s"].at[u], sems["z_r"].at[u], beside).wait_recv()
        value = quarter[u % 3, z]
        for d in range(NZ - 1):
            value = value + zrecv[u, d].astype(jnp.float32)
        bands = h * M + lax.broadcasted_iota(jnp.int32, value.shape, 2)
        count = occupied[partners[q, ka]]
        masked[u, y, z] = jnp.where(bands < count, value, 0.0).astype(jnp.bfloat16)
        for d in range(1, NZ):
            remote(
                masked.at[u, y, z],
                masked.at[u, y, z],
                sems["zz_s"].at[u],
                sems["zz_r"].at[u],
                (ka, y * NZ + z_peer(d)),
            ).start()

    def gather_z(u):
        if NZ > 1:
            block = masked.at[u, 0, pl.ds(0, NZ - 1)]
            remote(block, block, sems["zz_s"].at[u], sems["zz_r"].at[u], beside).wait_recv()
        for d in range(1, NY):
            remote(
                masked.at[u, y],
                masked.at[u, y],
                sems["yy_s"].at[u],
                sems["yy_r"].at[u],
                (ka, y_peer(d) * NZ + z),
            ).start()

    width = 256

    def columns(side, h):
        start = side * (H - 1) * M + h * M if h < H - 1 else (2 * (H - 1) + side) * M
        return slice(start, start + M)

    def gather_y(u):
        q, h = units[u]
        if NY > 1:
            block = masked.at[u, pl.ds(0, NY - 1)]
            remote(block, block, sems["yy_s"].at[u], sems["yy_r"].at[u], beside).wait_recv()
        real = masked[u, :, :, 0].reshape(B, M)
        imag = masked[u, :, :, 1].reshape(B, M)
        left, right = columns(0, h), columns(1, h)
        mixer[q, 0:B, left] = real
        mixer[q, 0:B, right] = -imag
        mixer[q, B : 2 * B, left] = imag
        mixer[q, B : 2 * B, right] = real

    def prepare(q):
        early = (H - 1) * M

        def strip(t, _):
            at = pl.ds(pl.multiple_of(t * width, width), width)
            orbits = partner[q, :, 0:early, at].reshape(2 * early, width)
            mixed = dot(mixer[q, :, 0 : 2 * early], orbits, ((1,), (0,)))
            part[q, :, at] = applied[q, :, at].astype(jnp.float32) - mixed
            return 0

        lax.fori_loop(0, G // width, strip, 0)

    def project(q):
        own_count = occupied[ka]
        def strip(t, _):
            at = pl.ds(pl.multiple_of(t * width, width), width)
            orbits = partner[q, :, (H - 1) * M : B, at].reshape(2 * M, width)
            mixed = dot(mixer[q, :, 2 * (H - 1) * M : 2 * B], orbits, ((1,), (0,)))
            real = part[q, 0:B, at] - mixed[:B]
            imag = part[q, B : 2 * B, at] - mixed[B:]
            sources[q, 0, 0, :, at] = real.astype(jnp.bfloat16)
            sources[q, 0, 1, :, at] = imag.astype(jnp.bfloat16)
            term = orbitals[0, :, at].astype(jnp.float32) * real
            term = term + orbitals[1, :, at].astype(jnp.float32) * imag
            bands = lax.broadcasted_iota(jnp.int32, term.shape, 0)
            term = jnp.where(bands < own_count, term, 0.0)
            shares[q, ka, :, at] = density_weight * jnp.sum(term, axis=0, keepdims=True)
            return 0

        lax.fori_loop(0, G // width, strip, 0)
        for d in range(1, K):
            remote(
                shares.at[q, ka],
                shares.at[q, ka],
                sems["share_s"].at[q],
                sems["share_r"].at[q],
                (lax.rem(ka + d, K), gr),
            ).start()

    def give(h):
        wait_relay(h)
        hand_out(h)

    count = len(units)
    start_relay(0)
    for load in loads[1:]:
        load.wait()
    apply_field(0)
    beat = 22.0 / H
    first = 30 + beat
    steps = [(13 + beat * h, 0, pass_on, h) for h in range(H)]
    steps += [(7 + 2 * beat * (h + 1), 1, give, h) for h in range(H)]
    steps += [(6 + beat * h, 2, start_relay, h) for h in range(1, H)]
    steps += [(7 + beat * q, 3, apply_field, q) for q in range(1, Q)]
    for u in range(count):
        arrives = first + beat * u
        steps += [(arrives, 4, intersect, u)]
        for i, (lag, step) in enumerate(zip(LAGS, (sum_y, sum_z, gather_z))):
            steps += [(arrives + lag, 5 + i, step, u)]
        q, h = units[u]
        gathered = arrives + GATHERED
        if h == H - 1:
            gathered = first + beat * (count - 1) + LAST[q]
        steps += [(gathered, 8, gather_y, u)]
        if h >= H - 2:
            steps += [(gathered + 0.01, 9, prepare if h == H - 2 else project, q)]
    for _, _, step, argument in sorted(steps, key=lambda entry: entry[:2] + entry[3:]):
        step(argument)

    for q in range(Q):
        block = shares.at[q, pl.ds(0, K - 1)]
        remote(block, block, sems["share_s"].at[q], sems["share_r"].at[q], beside).wait_recv()
        density[q : q + 1, :] = jnp.sum(shares[q], axis=0)

    def sent(block, sem):
        remote(block, block, sem, sem, beside).wait_send()

    for q in range(Q):
        sent(shares.at[q, pl.ds(0, K - 1)], sems["share_s"].at[q])
    for h in range(H):
        sent(held[h].at[pl.ds(0, J - 1)], sems["spread_s"].at[h])
        sent(held[h].at[pl.ds(0, J)], sems["relay_s"].at[h])
    for u in range(count):
        sent(picked.at[u], sems["hand_s"].at[u])
        if NY > 1:
            sent(yrecv.at[u], sems["y_s"].at[u])
            sent(masked.at[u, pl.ds(0, NY - 1)], sems["yy_s"].at[u])
        if NZ > 1:
            sent(zrecv.at[u], sems["z_s"].at[u])
            sent(masked.at[u, 0, pl.ds(0, NZ - 1)], sems["zz_s"].at[u])


def publish(sources, density, sources_out, density_out, sems):
    copies = [pltpu.make_async_copy(density, density_out, sems.at[0])]
    for i in range(2 * sources.shape[0]):
        q, part = divmod(i, 2)
        at = (q, 0, part)
        copies.append(pltpu.make_async_copy(sources.at[at], sources_out.at[at], sems.at[i + 1]))
    for copy in copies:
        copy.start()
    for copy in copies:
        copy.wait()


def shards(sizes, orbitals, potential, partners, occupied):
    K, NY, NZ, Q, H = sizes
    _, _, B, G = orbitals.shape
    J, M = K // 2, B // H
    R, YN = M // J, B // NY
    ZN, U = YN // NZ, Q * H
    half, full = jnp.bfloat16, jnp.float32
    DMA = pltpu.SemaphoreType.DMA
    sems = {name: DMA((U,)) for part in ("hand", "y", "z", "zz", "yy") for name in (part + "_s", part + "_r")}
    sems |= {"spread_s": DMA((H,)), "spread_r": DMA((H, J)), "relay_s": DMA((H,)), "relay_r": DMA((H,))}
    sems |= {"share_s": DMA((Q,)), "share_r": DMA((Q,)), "load": DMA((4,))}
    scratch = dict(
        partners=pltpu.SMEM((Q, K), jnp.int32),
        occupied=pltpu.SMEM((K,), jnp.int32),
        potential=pltpu.VMEM((Q, 2, G), full),
        orbitals=pltpu.VMEM((2, B, G), half),
        held=[pltpu.VMEM((K, 2, R, G), half) for _ in range(H)],
        picked=pltpu.VMEM((U, J - 1, 2, R, G), half),
        partner=pltpu.VMEM((Q, 2, B, G), half),
        applied=pltpu.VMEM((Q, 2 * B, G), half),
        whole=pltpu.VMEM((3, NY, 2, YN, M), full),
        ysend=pltpu.VMEM((U, NY, 2, YN, M), half),
        yrecv=pltpu.VMEM((U, max(NY - 1, 1), 2, YN, M), half),
        quarter=pltpu.VMEM((3, NZ, 2, ZN, M), full),
        zsend=pltpu.VMEM((U, NZ, 2, ZN, M), half),
        zrecv=pltpu.VMEM((U, max(NZ - 1, 1), 2, ZN, M), half),
        masked=pltpu.VMEM((U, NY, NZ, 2, ZN, M), half),
        mixer=pltpu.VMEM((Q, 2 * B, 2 * B), half),
        part=pltpu.VMEM((Q, 2 * B, G), full),
        shares=pltpu.VMEM((Q, K, 1, G), full),
        sems=sems,
    )
    vmem = pl.BlockSpec(memory_space=pltpu.VMEM)
    sources, density = pl.pallas_call(
        functools.partial(kernel, sizes),
        out_shape=(
            pltpu.VMEM((Q, 1, 2, B, G), half),
            pltpu.VMEM((Q, G), full),
        ),
        in_specs=[pl.BlockSpec(memory_space=pl.ANY)] * 4,
        out_specs=(vmem, vmem),
        scratch_shapes=scratch,
        compiler_params=pltpu.CompilerParams(
            collective_id=0, has_side_effects=True, vmem_limit_bytes=57 * 1024 * 1024
        ),
    )(partners, occupied, orbitals, potential)
    anywhere = pl.BlockSpec(memory_space=pl.ANY)
    return pl.pallas_call(
        publish,
        out_shape=(
            jax.ShapeDtypeStruct((Q, 1, 2, B, G), half),
            jax.ShapeDtypeStruct((Q, G), full),
        ),
        in_specs=[anywhere] * 2,
        out_specs=(anywhere, anywhere),
        scratch_shapes=[DMA((2 * Q + 1,))],
        compiler_params=pltpu.CompilerParams(vmem_limit_bytes=1024 * 1024),
    )(sources, density)


def solution(mesh, ways=None):
    K, points = mesh.shape["ka"], mesh.shape["grid"]
    NY, NZ = ways or (4, points // 4)

    def local(orbitals, potential, partners, occupied):
        sizes = (K, NY, NZ, potential.shape[0], BLOCKS)
        return shards(sizes, orbitals, potential, partners, occupied)

    return jax.shard_map(
        local,
        mesh=mesh,
        in_specs=(P("ka", None, None, "grid"), P(None, None, "grid"), P(), P()),
        out_specs=(P(None, "ka", None, None, "grid"), P(None, "grid")),
        check_vma=False,
    )
```

```python
import functools

import jax
import jax.numpy as jnp
from jax import lax
from jax.experimental import pallas as pl
from jax.experimental.pallas import tpu as pltpu
from jax.sharding import PartitionSpec as P

MESH = pl.DeviceIdType.MESH
BLOCKS = 4
LAGS = (10.0, 17.0, 25.0)
GATHERED = 35.0
LAST = (26.0, 30.0, 34.0)


def remote(src, dst, send_sem, recv_sem, target):
    return pltpu.make_async_remote_copy(
        src_ref=src,
        dst_ref=dst,
        send_sem=send_sem,
        recv_sem=recv_sem,
        device_id=target,
        device_id_type=MESH,
    )


def dot(a, b, dims):
    return lax.dot_general(a, b, (dims, ((), ())), preferred_element_type=jnp.float32)


def kernel(
    sizes,
    given_partners,
    given_occupied,
    given_orbitals,
    given_potential,
    sources,
    density,
    partners,
    occupied,
    potential,
    orbitals,
    held,
    picked,
    partner,
    applied,
    whole,
    ysend,
    yrecv,
    quarter,
    zsend,
    zrecv,
    masked,
    mixer,
    part,
    shares,
    sems,
):
    K, NY, NZ, Q, H = sizes
    _, B, G = orbitals.shape
    NX, J = K // 4, K // 2
    M = B // H
    R = M // J
    YN = B // NY
    ZN = YN // NZ
    volume_weight = 1.0 / (G * NY * NZ)
    density_weight = 2.0 / (K * B)
    units = [(q, h) for h in range(H) for q in range(Q)]

    ka = lax.axis_index("ka")
    gr = lax.axis_index("grid")
    x, low, core = lax.div(ka, 4), lax.rem(lax.div(ka, 2), 2), lax.rem(ka, 2)
    y, z = lax.div(gr, NZ), lax.rem(gr, NZ)

    order = [(0, 1)]
    for dx in [1, NX - 1, 2]:
        for dc in (0, 1):
            if 0 < dx < NX and (dx, dc) not in order:
                order.append((dx, dc))

    def plane(dx, dc):
        px, pc = lax.rem(x + dx + NX, NX), lax.rem(core + dc + 2, 2)
        return px * 4 + low * 2 + pc, px * 2 + pc

    mine = x * 2 + core
    beside = (x * 4 + (1 - low) * 2 + core, gr)

    def y_peer(d):
        return lax.rem(y + d, NY)

    def z_peer(d):
        return lax.rem(z + d, NZ)

    barrier = pltpu.get_barrier_semaphore()
    greeted = [(lax.rem(ka + d, K), gr) for d in range(1, K)]
    greeted += [(ka, y_peer(d) * NZ + z) for d in range(1, NY)]
    greeted += [(ka, y * NZ + z_peer(d)) for d in range(1, NZ)]
    for target in greeted:
        pl.semaphore_signal(barrier, inc=1, device_id=target, device_id_type=MESH)
    loads = [
        pltpu.make_async_copy(src, dst, sems["load"].at[i])
        for i, (src, dst) in enumerate(
            [
                (given_orbitals.at[0], orbitals),
                (given_potential, potential),
                (given_partners, partners),
                (given_occupied, occupied),
            ]
        )
    ]
    for load in loads:
        load.start()
    pl.semaphore_wait(barrier, len(greeted))
    loads[0].wait()

    def rows(h, piece):
        return pl.ds(pl.multiple_of(h * M + piece * R, R), R)

    for h in range(H):
        for i, (dx, dc) in enumerate(order):
            pk, pj = plane(dx, dc)
            remote(
                orbitals.at[:, rows(h, pj), :],
                held[h].at[ka],
                sems["spread_s"].at[h],
                sems["spread_r"].at[h, i],
                (pk, gr),
            ).start()

    def apply_field(q):
        real, imag = potential[q, 0:1, :], potential[q, 1:2, :]

        def strip(t, _):
            at = pl.ds(pl.multiple_of(t * 64, 64), 64)
            under = pl.ds(pl.multiple_of(B + t * 64, 64), 64)
            own_real = orbitals[0, at, :].astype(jnp.float32)
            own_imag = orbitals[1, at, :].astype(jnp.float32)
            applied[q, at, :] = (real * own_real - imag * own_imag).astype(jnp.bfloat16)
            applied[q, under, :] = (real * own_imag + imag * own_real).astype(jnp.bfloat16)
            return 0

        lax.fori_loop(0, B // 64, strip, 0)

    def relay(h, slot, source):
        remote(
            source, held[h].at[slot], sems["relay_s"].at[h], sems["relay_r"].at[h], beside
        ).start()

    def start_relay(h):
        relay(h, ka, orbitals.at[:, rows(h, mine), :])
        held[h][ka] = orbitals[:, rows(h, mine), :]

    def pass_on(h):
        for i, (dx, dc) in enumerate(order):
            slot, _ = plane(-dx, -dc)
            remote(
                held[h].at[slot],
                held[h].at[slot],
                sems["spread_s"].at[h],
                sems["spread_r"].at[h, i],
                beside,
            ).wait_recv()
            relay(h, slot, held[h].at[slot])

    def wait_relay(h):
        block = held[h].at[pl.ds(0, J)]
        remote(block, block, sems["relay_s"].at[h], sems["relay_r"].at[h], beside).wait_recv()

    def hand_out(h):
        for q in range(Q):
            u = h * Q + q
            for i, (dx, dc) in enumerate(order):
                pk, _ = plane(dx, dc)
                picked[u, i] = held[h][partners[q, pk]]
            partner[q, :, rows(h, mine), :] = held[h][partners[q, ka]]
            for i, (dx, dc) in enumerate(order):
                pk, _ = plane(dx, dc)
                remote(
                    picked.at[u, i],
                    partner.at[q, :, rows(h, mine), :],
                    sems["hand_s"].at[u],
                    sems["hand_r"].at[u],
                    (pk, gr),
                ).start()

    def intersect(u):
        q, h = units[u]
        block = partner.at[q, :, pl.ds(h * M, (J - 1) * R), :]
        remote(block, block, sems["hand_s"].at[u], sems["hand_r"].at[u], beside).wait_recv()
        last = ((1,), (1,))
        orbits = partner[q, :, h * M : (h + 1) * M, :].reshape(2 * M, G)
        both = dot(applied[q], orbits, last)
        real = volume_weight * (both[:B, :M] + both[B:, M:])
        imag = volume_weight * (both[B:, :M] - both[:B, M:])
        for part, value in enumerate((real, imag)):
            value = value.reshape(NY, YN, M)
            whole[u % 3, :, part] = value
            ysend[u, :, part] = value.astype(jnp.bfloat16)
        for d in range(1, NY):
            remote(
                ysend.at[u, y_peer(d)],
                yrecv.at[u, d - 1],
                sems["y_s"].at[u],
                sems["y_r"].at[u],
                (ka, y_peer(d) * NZ + z),
            ).start()

    def sum_y(u):
        if NY > 1:
            block = yrecv.at[u]
            remote(block, block, sems["y_s"].at[u], sems["y_r"].at[u], beside).wait_recv()
        for t in range(NZ):
            value = whole[u % 3, y, :, t * ZN : (t + 1) * ZN, :]
            for d in range(NY - 1):
                value = value + yrecv[u, d, :, t * ZN : (t + 1) * ZN, :].astype(jnp.float32)
            quarter[u % 3, t] = value
            zsend[u, t] = value.astype(jnp.bfloat16)
        for d in range(1, NZ):
            remote(
                zsend.at[u, z_peer(d)],
                zrecv.at[u, d - 1],
                sems["z_s"].at[u],
                sems["z_r"].at[u],
                (ka, y * NZ + z_peer(d)),
            ).start()

    def sum_z(u):
        q, h = units[u]
        if NZ > 1:
            block = zrecv.at[u]
            remote(block, block, sems["z_s"].at[u], sems["z_r"].at[u], beside).wait_recv()
        value = quarter[u % 3, z]
        for d in range(NZ - 1):
            value = value + zrecv[u, d].astype(jnp.float32)
        bands = h * M + lax.broadcasted_iota(jnp.int32, value.shape, 2)
        count = occupied[partners[q, ka]]
        masked[u, y, z] = jnp.where(bands < count, value, 0.0).astype(jnp.bfloat16)
        for d in range(1, NZ):
            remote(
                masked.at[u, y, z],
                masked.at[u, y, z],
                sems["zz_s"].at[u],
                sems["zz_r"].at[u],
                (ka, y * NZ + z_peer(d)),
            ).start()

    def gather_z(u):
        if NZ > 1:
            block = masked.at[u, 0, pl.ds(0, NZ - 1)]
            remote(block, block, sems["zz_s"].at[u], sems["zz_r"].at[u], beside).wait_recv()
        for d in range(1, NY):
            remote(
                masked.at[u, y],
                masked.at[u, y],
                sems["yy_s"].at[u],
                sems["yy_r"].at[u],
                (ka, y_peer(d) * NZ + z),
            ).start()

    width = 256

    def columns(side, h):
        start = side * (H - 1) * M + h * M if h < H - 1 else (2 * (H - 1) + side) * M
        return slice(start, start + M)

    def gather_y(u):
        q, h = units[u]
        if NY > 1:
            block = masked.at[u, pl.ds(0, NY - 1)]
            remote(block, block, sems["yy_s"].at[u], sems["yy_r"].at[u], beside).wait_recv()
        real = masked[u, :, :, 0].reshape(B, M)
        imag = masked[u, :, :, 1].reshape(B, M)
        left, right = columns(0, h), columns(1, h)
        mixer[q, 0:B, left] = real
        mixer[q, 0:B, right] = -imag
        mixer[q, B : 2 * B, left] = imag
        mixer[q, B : 2 * B, right] = real

    def prepare(q):
        early = (H - 1) * M

        def strip(t, _):
            at = pl.ds(pl.multiple_of(t * width, width), width)
            orbits = partner[q, :, 0:early, at].reshape(2 * early, width)
            mixed = dot(mixer[q, :, 0 : 2 * early], orbits, ((1,), (0,)))
            part[q, :, at] = applied[q, :, at].astype(jnp.float32) - mixed
            return 0

        lax.fori_loop(0, G // width, strip, 0)

    def project(q):
        own_count = occupied[ka]
        def strip(t, _):
            at = pl.ds(pl.multiple_of(t * width, width), width)
            orbits = partner[q, :, (H - 1) * M : B, at].reshape(2 * M, width)
            mixed = dot(mixer[q, :, 2 * (H - 1) * M : 2 * B], orbits, ((1,), (0,)))
            real = part[q, 0:B, at] - mixed[:B]
            imag = part[q, B : 2 * B, at] - mixed[B:]
            sources[q, 0, 0, :, at] = real.astype(jnp.bfloat16)
            sources[q, 0, 1, :, at] = imag.astype(jnp.bfloat16)
            term = orbitals[0, :, at].astype(jnp.float32) * real
            term = term + orbitals[1, :, at].astype(jnp.float32) * imag
            bands = lax.broadcasted_iota(jnp.int32, term.shape, 0)
            term = jnp.where(bands < own_count, term, 0.0)
            shares[q, ka, :, at] = density_weight * jnp.sum(term, axis=0, keepdims=True)
            return 0

        lax.fori_loop(0, G // width, strip, 0)
        for d in range(1, K):
            remote(
                shares.at[q, ka],
                shares.at[q, ka],
                sems["share_s"].at[q],
                sems["share_r"].at[q],
                (lax.rem(ka + d, K), gr),
            ).start()

    def give(h):
        wait_relay(h)
        hand_out(h)

    count = len(units)
    start_relay(0)
    for load in loads[1:]:
        load.wait()
    apply_field(0)
    beat = 22.0 / H
    first = 30 + beat
    steps = [(13 + beat * h, 0, pass_on, h) for h in range(H)]
    steps += [(7 + 2 * beat * (h + 1), 1, give, h) for h in range(H)]
    steps += [(6 + beat * h, 2, start_relay, h) for h in range(1, H)]
    steps += [(7 + beat * q, 3, apply_field, q) for q in range(1, Q)]
    for u in range(count):
        arrives = first + beat * u
        steps += [(arrives, 4, intersect, u)]
        for i, (lag, step) in enumerate(zip(LAGS, (sum_y, sum_z, gather_z))):
            steps += [(arrives + lag, 5 + i, step, u)]
        q, h = units[u]
        gathered = arrives + GATHERED
        if h == H - 1:
            gathered = first + beat * (count - 1) + LAST[q]
        steps += [(gathered, 8, gather_y, u)]
        if h >= H - 2:
            steps += [(gathered + 0.01, 9, prepare if h == H - 2 else project, q)]
    for _, _, step, argument in sorted(steps, key=lambda entry: entry[:2] + entry[3:]):
        step(argument)

    def sent(block, sem):
        remote(block, block, sem, sem, beside).wait_send()

    for h in range(H):
        sent(held[h].at[pl.ds(0, J - 1)], sems["spread_s"].at[h])
        sent(held[h].at[pl.ds(0, J)], sems["relay_s"].at[h])
    for u in range(count):
        sent(picked.at[u], sems["hand_s"].at[u])
        if NY > 1:
            sent(yrecv.at[u], sems["y_s"].at[u])
            sent(masked.at[u, pl.ds(0, NY - 1)], sems["yy_s"].at[u])
        if NZ > 1:
            sent(zrecv.at[u], sems["z_s"].at[u])
            sent(masked.at[u, 0, pl.ds(0, NZ - 1)], sems["zz_s"].at[u])

    for q in range(Q):
        block = shares.at[q, pl.ds(0, K - 1)]
        remote(block, block, sems["share_s"].at[q], sems["share_r"].at[q], beside).wait_recv()
        density[q : q + 1, :] = jnp.sum(shares[q], axis=0)
    for q in range(Q):
        sent(shares.at[q, pl.ds(0, K - 1)], sems["share_s"].at[q])


def publish(sources, density, sources_out, density_out, sems):
    copies = [pltpu.make_async_copy(density, density_out, sems.at[0])]
    for i in range(2 * sources.shape[0]):
        q, part = divmod(i, 2)
        at = (q, 0, part)
        copies.append(pltpu.make_async_copy(sources.at[at], sources_out.at[at], sems.at[i + 1]))
    for copy in copies:
        copy.start()
    for copy in copies:
        copy.wait()


def shards(sizes, orbitals, potential, partners, occupied):
    K, NY, NZ, Q, H = sizes
    _, _, B, G = orbitals.shape
    J, M = K // 2, B // H
    R, YN = M // J, B // NY
    ZN, U = YN // NZ, Q * H
    half, full = jnp.bfloat16, jnp.float32
    DMA = pltpu.SemaphoreType.DMA
    sems = {name: DMA((U,)) for part in ("hand", "y", "z", "zz", "yy") for name in (part + "_s", part + "_r")}
    sems |= {"spread_s": DMA((H,)), "spread_r": DMA((H, J)), "relay_s": DMA((H,)), "relay_r": DMA((H,))}
    sems |= {"share_s": DMA((Q,)), "share_r": DMA((Q,)), "load": DMA((4,))}
    scratch = dict(
        partners=pltpu.SMEM((Q, K), jnp.int32),
        occupied=pltpu.SMEM((K,), jnp.int32),
        potential=pltpu.VMEM((Q, 2, G), full),
        orbitals=pltpu.VMEM((2, B, G), half),
        held=[pltpu.VMEM((K, 2, R, G), half) for _ in range(H)],
        picked=pltpu.VMEM((U, J - 1, 2, R, G), half),
        partner=pltpu.VMEM((Q, 2, B, G), half),
        applied=pltpu.VMEM((Q, 2 * B, G), half),
        whole=pltpu.VMEM((3, NY, 2, YN, M), full),
        ysend=pltpu.VMEM((U, NY, 2, YN, M), half),
        yrecv=pltpu.VMEM((U, max(NY - 1, 1), 2, YN, M), half),
        quarter=pltpu.VMEM((3, NZ, 2, ZN, M), full),
        zsend=pltpu.VMEM((U, NZ, 2, ZN, M), half),
        zrecv=pltpu.VMEM((U, max(NZ - 1, 1), 2, ZN, M), half),
        masked=pltpu.VMEM((U, NY, NZ, 2, ZN, M), half),
        mixer=pltpu.VMEM((Q, 2 * B, 2 * B), half),
        part=pltpu.VMEM((Q, 2 * B, G), full),
        shares=pltpu.VMEM((Q, K, 1, G), full),
        sems=sems,
    )
    vmem = pl.BlockSpec(memory_space=pltpu.VMEM)
    sources, density = pl.pallas_call(
        functools.partial(kernel, sizes),
        out_shape=(
            pltpu.VMEM((Q, 1, 2, B, G), half),
            pltpu.VMEM((Q, G), full),
        ),
        in_specs=[pl.BlockSpec(memory_space=pl.ANY)] * 4,
        out_specs=(vmem, vmem),
        scratch_shapes=scratch,
        compiler_params=pltpu.CompilerParams(
            collective_id=0, has_side_effects=True, vmem_limit_bytes=57 * 1024 * 1024
        ),
    )(partners, occupied, orbitals, potential)
    anywhere = pl.BlockSpec(memory_space=pl.ANY)
    return pl.pallas_call(
        publish,
        out_shape=(
            jax.ShapeDtypeStruct((Q, 1, 2, B, G), half),
            jax.ShapeDtypeStruct((Q, G), full),
        ),
        in_specs=[anywhere] * 2,
        out_specs=(anywhere, anywhere),
        scratch_shapes=[DMA((2 * Q + 1,))],
        compiler_params=pltpu.CompilerParams(vmem_limit_bytes=1024 * 1024),
    )(sources, density)


def solution(mesh, ways=None):
    K, points = mesh.shape["ka"], mesh.shape["grid"]
    NY, NZ = ways or (4, points // 4)

    def local(orbitals, potential, partners, occupied):
        sizes = (K, NY, NZ, potential.shape[0], BLOCKS)
        return shards(sizes, orbitals, potential, partners, occupied)

    return jax.shard_map(
        local,
        mesh=mesh,
        in_specs=(P("ka", None, None, "grid"), P(None, None, "grid"), P(), P()),
        out_specs=(P(None, "ka", None, None, "grid"), P(None, "grid")),
        check_vma=False,
    )
```
